8 devices in a mesh: rep: 1 (over z), dp: 8 (over x, y, core).
Axes of the slice: x: 2, y: 2, z: 1, core: 2. Of those that a mesh axis runs over, the one named last changes fastest.
Arguments:
- x: bfloat16 [8, 2048, 896], P(('rep', 'dp'))
- dy: bfloat16 [8, 2048, 896], P(('rep', 'dp'))
- w_gate: bfloat16 [2, 896, 2560], replicated
- w_up: bfloat16 [2, 896, 2560], replicated
- w_down: bfloat16 [2, 2560, 896], replicated
- m_w_gate: float32 [2, 896, 2560], replicated
- m_w_up: float32 [2, 896, 2560], replicated
- m_w_down: float32 [2, 2560, 896], replicated
- v_w_gate: float32 [2, 896, 2560], replicated
- v_w_up: float32 [2, 896, 2560], replicated
- v_w_down: float32 [2, 2560, 896], replicated
Outputs:
- output 1: bfloat16 [2, 896, 2560], P('rep')
- output 2: bfloat16 [2, 896, 2560], P('rep')
- output 3: bfloat16 [2, 2560, 896], P('rep')
- output 4: float32 [2, 896, 2560], P('rep')
- output 5: float32 [2, 896, 2560], P('rep')
- output 6: float32 [2, 2560, 896], P('rep')
- output 7: float32 [2, 896, 2560], P('rep')
- output 8: float32 [2, 896, 2560], P('rep')
- output 9: float32 [2, 2560, 896], P('rep')
All inputs are finite; a program needn't handle non-finite values.
Results may differ from the reference program's by a relative error of at most 0.022.
Values are sent between devices in bfloat16 or wider.
A program may use at most 2.5 GiB of HBM per device.

```python
import jax
import jax.numpy as jnp
from jax import lax

SEQUENCES = 8
TOKENS = 2048
D = 896
FF = 2560
LAYERS = 2
NAMES = ("w_gate", "w_up", "w_down")
SHAPES = {"w_gate": (LAYERS, D, FF), "w_up": (LAYERS, D, FF), "w_down": (LAYERS, FF, D)}


def bump(key, n, height):
    away = (jnp.arange(n, dtype=jnp.int32) - jax.random.randint(key, (), 0, n, jnp.int32)) % n
    return jnp.where(away < n // 8, height, 1.0)


def together(key, own, strength):
    shared = jax.random.normal(key, own.shape[1:], jnp.float32)
    return (own + strength * shared) * lax.rsqrt(1 + strength * strength)


def setup_inputs(seed: int = 0, part: int = 0) -> dict:
    kx, kdy, ka, kb, kz, kf, kh, kl, *keys = jax.random.split(jax.random.key(seed), 8 + 3 * len(NAMES))
    kx, kdy, ka, kb = (jax.random.fold_in(k, part) for k in (kx, kdy, ka, kb))
    kw, km, kv = (keys[i::3] for i in range(3))
    shape = (SEQUENCES, TOKENS, D)
    much_x, much_dy = jax.random.uniform(kz, (2,), jnp.float32, 0.0, 1.0)
    loud = 2.0 ** jax.random.uniform(jax.random.fold_in(kz, 1), (), jnp.float32, -1.0, 2.0)
    layers = 2.0 ** jax.random.uniform(kl, (LAYERS, 1, 1), jnp.float32, -1.0, 1.0)
    x = together(ka, jax.random.normal(kx, shape, jnp.float32), much_x) * bump(kf, D, 4.0)
    dy = together(kb, jax.random.normal(kdy, shape, jnp.float32), much_dy)
    drawn = {"x": x.astype(jnp.bfloat16), "dy": (loud * dy * (SEQUENCES * TOKENS) ** -0.5).astype(jnp.bfloat16)}
    for key, name in zip(kw, NAMES, strict=True):
        w = jax.random.normal(key, SHAPES[name], jnp.float32) * SHAPES[name][1] ** -0.5
        drawn[name] = (w * {"w_gate": 1.0, "w_up": bump(kh, FF, 4.0), "w_down": layers}[name]).astype(jnp.bfloat16)
    for key, name in zip(km, NAMES, strict=True):
        drawn[f"m_{name}"] = 0.1 * jax.random.normal(key, SHAPES[name], jnp.float32)
    for key, name in zip(kv, NAMES, strict=True):
        drawn[f"v_{name}"] = jax.random.uniform(key, SHAPES[name], jnp.float32, 0.005, 0.015)
    return drawn


def matmul(a, w):
    return jnp.dot(a, w, preferred_element_type=jnp.float32).astype(jnp.bfloat16)


def normed(h):
    wide = h.astype(jnp.float32)
    scale = lax.rsqrt(jnp.mean(wide**2, -1, keepdims=True) + 1e-6)
    return (wide * scale).astype(jnp.bfloat16)


def layer(h, w):
    a = normed(h)
    gate = jnp.dot(a, w["w_gate"], preferred_element_type=jnp.float32)
    up = jnp.dot(a, w["w_up"], preferred_element_type=jnp.float32)
    return h + matmul((jax.nn.silu(gate) * up).astype(jnp.bfloat16), w["w_down"])


def adamw(w, m, v, g):
    m = 0.9 * m + 0.1 * g
    v = 0.95 * v + 0.05 * g * g
    step = m * lax.rsqrt(v + 1e-8) + 0.1 * w
    return (w - 0.02 * step).astype(jnp.bfloat16), m, v


def clipped(gradients, sum_of_squares, count):
    factor = jnp.minimum(1.0, 0.5 * lax.rsqrt(sum_of_squares / count + 1e-30))
    return [g * factor for g in gradients]


def stack(weights, h):
    return lax.scan(lambda h, w: (layer(h, w), None), h, weights)[0]


def reference(x, dy, w_gate, w_up, w_down, m_w_gate, m_w_up, m_w_down, v_w_gate, v_w_up, v_w_down):
    weights = dict(zip(NAMES, (w_gate, w_up, w_down), strict=True))

    def take(so_far, sequence):
        h, by_y = sequence
        _, back = jax.vjp(lambda w: stack(w, h), weights)
        return jax.tree.map(lambda total, term: total + term.astype(jnp.float32), so_far, back(by_y)[0]), None

    none_yet = {name: jnp.zeros(w.shape, jnp.float32) for name, w in weights.items()}
    by_weights, _ = lax.scan(take, none_yet, (x, dy))
    gradients = [by_weights[name].astype(jnp.bfloat16).astype(jnp.float32) for name in NAMES]
    gradients = clipped(gradients, sum(jnp.sum(g * g) for g in gradients), sum(g.size for g in gradients))
    new = [
        adamw(w.astype(jnp.float32), m, v, g)
        for w, m, v, g in zip((w_gate, w_up, w_down), (m_w_gate, m_w_up, m_w_down), (v_w_gate, v_w_up, v_w_down), gradients, strict=True)
    ]
    return tuple(one[which] for which in range(3) for one in new)
```

```python
import functools

import jax
import jax.numpy as jnp
from jax import lax
from jax.experimental import pallas as pl
from jax.experimental.pallas import tpu as pltpu
from jax.sharding import PartitionSpec as P

MESH = pl.DeviceIdType.MESH
F32, BF16 = jnp.float32, jnp.bfloat16
T = 256
RB = 512
NB = 256
VMEM_LIMIT = 63 * 1024 * 1024
TF = 512
GATHERED = 10
CHUNKS = (5, 5)
SLOTS = 4
LAST = 2


def dot(a, b):
    return jnp.dot(a, b, preferred_element_type=F32)


def dot_nt(a, b):
    return lax.dot_general(a, b, (((1,), (1,)), ((), ())), preferred_element_type=F32)


def dot_tn(a, b):
    return lax.dot_general(a, b, (((0,), (0,)), ((), ())), preferred_element_type=F32)


def norm_scale(wide):
    return lax.rsqrt(jnp.mean(wide * wide, -1, keepdims=True) + 1e-6)


def forward_kernel(x_ref, wg_ref, wu_ref, wd_ref, gate_ref, up_ref, h_ref, a_ref, acc_ref):
    s = pl.program_id(0)
    tokens = x_ref.shape[0]

    @pl.when(s == 0)
    def _():
        def block(i, _):
            rows = pl.ds(pl.multiple_of(i * NB, NB), NB)
            wide = x_ref[rows, :].astype(F32)
            a_ref[rows, :] = (wide * norm_scale(wide)).astype(BF16)
            acc_ref[rows, :] = jnp.zeros((NB, acc_ref.shape[1]), F32)
            return 0

        lax.fori_loop(0, tokens // NB, block, 0)

    wg, wu, wd = wg_ref[0], wu_ref[0], wd_ref[0]
    for r in range(tokens // RB):
        rows = pl.ds(r * RB, RB)
        a = a_ref[rows, :]
        gate = dot(a, wg)
        up = dot(a, wu)
        for part in range(TF // T):
            gate_ref[part, rows, :] = gate[:, part * T : part * T + T]
            up_ref[part, rows, :] = up[:, part * T : part * T + T]
        act = (gate * jax.nn.sigmoid(gate) * up).astype(BF16)
        acc_ref[rows, :] += dot(act, wd)

    @pl.when(s == pl.num_programs(0) - 1)
    def _():
        def block(i, _):
            rows = pl.ds(pl.multiple_of(i * NB, NB), NB)
            h_ref[rows, :] = x_ref[rows, :] + acc_ref[rows, :].astype(BF16)
            return 0

        lax.fori_loop(0, tokens // NB, block, 0)


def forward(x, w_gate, w_up, w_down):
    tokens, d = x.shape
    ff = w_gate.shape[2]
    kept = jax.ShapeDtypeStruct((ff // T, tokens, T), F32)
    keep = pl.BlockSpec((TF // T, tokens, T), lambda s: (s, 0, 0))
    return pl.pallas_call(
        forward_kernel,
        grid=(ff // TF,),
        out_shape=(kept, kept, jax.ShapeDtypeStruct((tokens, d), BF16)),
        in_specs=[
            pl.BlockSpec((tokens, d), lambda s: (0, 0), pipeline_mode=pl.Buffered(1)),
            pl.BlockSpec((1, d, TF), lambda s: (0, 0, s)),
            pl.BlockSpec((1, d, TF), lambda s: (0, 0, s)),
            pl.BlockSpec((1, TF, d), lambda s: (0, s, 0)),
        ],
        out_specs=(keep, keep, pl.BlockSpec((tokens, d), lambda s: (0, 0))),
        scratch_shapes=[pltpu.VMEM((tokens, d), BF16), pltpu.VMEM((tokens, d), F32)],
        compiler_params=pltpu.CompilerParams(dimension_semantics=("arbitrary",), vmem_limit_bytes=VMEM_LIMIT),
        cost_estimate=pl.CostEstimate(flops=6 * tokens * d * ff, bytes_accessed=64 << 20, transcendentals=0),
        name="forward_layer",
    )(x, w_gate, w_up, w_down)


def down_rows(which, share):
    return 128 * (share // 4) + 64 * which + 16 * (share % 4)


def backward_kernel(
    n, count, x_hbm, h_hbm, dy_hbm, wg_ref, wu_ref, wd_ref, gate_ref, up_ref, share_ref, factor_ref, full,
    h, d, a, at, dat, act, dgu, g, s1, r1, s2, r2, k2, s3, r3, k3, ssv, ssall,
    load_sem, own_sem, send_sem, recv_sem, ss_send, ss_recv,
):
    s = pl.program_id(0)
    me = lax.axis_index("dp")
    c, y, x = lax.rem(me, 2), lax.rem(me // 2, 2), me // 4
    over_c, over_y, over_x = me + 1 - 2 * c, me + 2 - 4 * y, me + 4 - 8 * x
    tokens, width = h.shape
    half, q2, q3 = width // 2, width // 4, width // 8

    def copy(src, dst, index, slot, target):
        return pltpu.make_async_remote_copy(
            src_ref=src, dst_ref=dst, send_sem=send_sem.at[index, slot], recv_sem=recv_sem.at[index, slot],
            device_id={"dp": target}, device_id_type=MESH,
        )

    def rows_at(start, size):
        return pl.ds(pl.multiple_of(start, size), size)

    def stage1(k):
        slot = lax.rem(k, 2)
        return [copy(s1.at[slot], r1.at[slot], 0, slot, over_c)]

    def stage2(k):
        slot = lax.rem(k, SLOTS)
        return [copy(s2.at[slot, i], r2.at[slot, i], 1 + i, slot, (over_x, over_y)[i]) for i in range(2)]

    def stage3(k):
        slot = lax.rem(k, SLOTS)
        return [copy(s3.at[slot, i], r3.at[slot, i], 3 + i, slot, (over_y, over_x)[i]) for i in range(2)]

    shares = (4 * c + 2 * x + y, 4 * c + 2 * y + x)

    def own(k):
        slot = lax.rem(k, SLOTS)
        return [
            pltpu.make_async_copy(share_ref.at[k, i], full.at[k, i, rows_at(shares[i] * q3, q3)], own_sem.at[i, slot]) for i in range(2)
        ]

    def gather1(k):
        slot = lax.rem(k, SLOTS)
        return [
            copy(share_ref.at[k, i], full.at[k, i, rows_at(shares[i] * q3, q3)], 5 + i, slot, (over_y, over_x)[i]) for i in range(2)
        ]

    def gather2(k):
        slot = lax.rem(k, SLOTS)
        parts = [full.at[k, i, rows_at((2 * c + (x, y)[i]) * q2, q2)] for i in range(2)]
        return [copy(parts[i], parts[i], 7 + i, slot, (over_x, over_y)[i]) for i in range(2)]

    def gather3(k):
        slot = lax.rem(k, SLOTS)
        parts = [full.at[k, i, rows_at(c * half, half)] for i in range(2)]
        return [copy(parts[i], parts[i], 9 + i, slot, over_c) for i in range(2)]

    def start(copies):
        for one in copies:
            one.start()

    def wait(copies):
        for one in copies:
            one.wait()

    def finish(k):
        slot = lax.rem(k, SLOTS)
        for i in range(2):
            one = (k3[slot, i] + r3[slot, i].astype(F32)).astype(BF16)
            share_ref[k, i] = one
            one = one.astype(F32)
            ssv[...] += jnp.sum((one * one).reshape(q3 // 8, 8, one.shape[1]), axis=0)

    def third(k):
        slot = lax.rem(k, SLOTS)
        for i, mine in enumerate((y, x)):
            away, here = rows_at((1 - mine) * q3, q3), rows_at(mine * q3, q3)
            s3[slot, i] = (k2[slot, i, away, :] + r2[slot, i, away, :].astype(F32)).astype(BF16)
            k3[slot, i] = k2[slot, i, here, :] + r2[slot, i, here, :].astype(F32)

    def second(k):
        slot, old = lax.rem(k, SLOTS), lax.rem(k, 2)
        for i, mine in enumerate((x, y)):
            away, here = rows_at((1 - mine) * q2, q2), rows_at(mine * q2, q2)
            s2[slot, i] = (g[i, rows_at((2 * c + 1 - mine) * q2, q2), :] + r1[old, i, away, :].astype(F32)).astype(BF16)
            k2[slot, i] = g[i, rows_at((2 * c + mine) * q2, q2), :] + r1[old, i, here, :].astype(F32)

    def exchange(step):
        def at_tile(lag, count, f):
            k = step - lag

            @pl.when((k >= 0) & (k < count))
            def _():
                f(k)

        if GATHERED:
            at_tile(11, GATHERED, lambda k: wait(gather3(k)))
            at_tile(9, GATHERED, lambda k: (wait(gather2(k)), start(gather3(k))))
            at_tile(7, GATHERED, lambda k: (wait(own(k) + gather1(k)), start(gather2(k))))
        at_tile(5, 2 * n, lambda k: (wait(stage3(k)), finish(k)))
        if GATHERED:
            at_tile(5, GATHERED, lambda k: start(own(k) + gather1(k)))
        at_tile(3, 2 * n, lambda k: (wait(stage2(k)), third(k), start(stage3(k))))
        at_tile(1, 2 * n, lambda k: (wait(stage1(k)), second(k), start(stage2(k))))

    def normed_rows(i, _):
        rows = rows_at(i * NB, NB)
        wide = h[rows, :].astype(F32)
        one = (wide * norm_scale(wide)).astype(BF16)
        a[rows, :] = one
        at[:, rows] = one.T
        return 0

    def load(src, dst, index):
        return pltpu.make_async_copy(src, dst, load_sem.at[index])

    @pl.when(s == 0)
    def _():
        barrier = pltpu.get_barrier_semaphore()
        load(h_hbm, h, 0).start()
        load(dy_hbm, d, 1).start()
        for other in range(1, 8):
            pl.semaphore_signal(barrier, inc=1, device_id={"dp": lax.rem(me + other, 8)}, device_id_type=MESH)
        ssv[...] = jnp.zeros_like(ssv)
        dat[...] = jnp.zeros_like(dat)
        load(h_hbm, h, 0).wait()
        lax.fori_loop(0, tokens // NB, normed_rows, 0)
        load(dy_hbm, d, 1).wait()
        pl.semaphore_wait(barrier, 7)

    exchange(s)

    def derive(rows, gate, up, dact):
        sig = jax.nn.sigmoid(gate)
        silu = gate * sig
        dact = dact.astype(BF16).astype(F32)
        act[rows, :] = (silu * up).astype(BF16)
        dgu[rows, :T] = (dact * up * (sig * (1.0 + gate * (1.0 - sig)))).astype(BF16)
        dgu[rows, T:] = (dact * silu).astype(BF16)

    def weight_gradients():
        both = dot(at[...], dgu[...])
        g[0, :, :T] = both[:, :T]
        g[1, :, :T] = both[:, T:]
        down = dot_tn(act[...], d[...])
        for which in range(2):
            for share in range(8):
                row = down_rows(which, share)
                for j in range(width // 128):
                    g[which, share * q3 + 16 * j : share * q3 + 16 * j + 16, T:] = down[row : row + 16, 128 * j : 128 * j + 128]
        s1[lax.rem(s, 2)] = g[:, rows_at((1 - c) * half, half), :].astype(BF16)
        start(stage1(s))

    blocks = [pl.ds(r * RB, RB) for r in range(tokens // RB)]

    @pl.when(s < n)
    def _():
        wgu = jnp.concatenate([wg_ref[0], wu_ref[0]], axis=1)
        wd = wd_ref[0]
        for rows in blocks:
            both = dot(a[rows, :], wgu)
            derive(rows, both[:, :T], both[:, T:], dot_nt(d[rows, :], wd))
        weight_gradients()
        for rows in blocks:
            dat[:, rows] += dot_nt(wgu, dgu[rows, :])

    @pl.when(s >= n)
    def _():
        wd = wd_ref[0]
        for rows in blocks:
            derive(rows, gate_ref[0, rows, :], up_ref[0, rows, :], dot_nt(d[rows, :], wd))
        weight_gradients()

    @pl.when(s == n - 1)
    def _():
        def block(i, _):
            rows = rows_at(i * NB, NB)
            wide = h[rows, :].astype(F32)
            scale = norm_scale(wide)
            by_a = dat[:, rows].T.astype(BF16).astype(F32)
            inner = jnp.mean(by_a * wide, -1, keepdims=True)
            by_h = by_a * scale - wide * (scale * scale * scale * inner)
            d[rows, :] = d[rows, :] + by_h.astype(BF16)
            return 0

        lax.fori_loop(0, tokens // NB, block, 0)
        load(x_hbm, h, 0).start()
        load(x_hbm, h, 0).wait()
        lax.fori_loop(0, tokens // NB, normed_rows, 0)

    @pl.when(s == 2 * n - 1)
    def _():
        def drain(step, _):
            exchange(step)
            return 0

        lax.fori_loop(2 * n, 2 * n + 5, drain, 0)
        ssall[0] = ssv[...]
        others = []
        for other in range(1, 8):
            others.append(
                pltpu.make_async_remote_copy(
                    src_ref=ssv, dst_ref=ssall.at[other], send_sem=ss_send.at[other], recv_sem=ss_recv.at[other],
                    device_id={"dp": lax.rem(me + other, 8)}, device_id_type=MESH,
                )
            )
        start(others)
        wait(others)
        total = ssall[me]
        for device in range(1, 8):
            total = total + ssall[lax.rem(me - device + 8, 8)]
        total = jnp.sum(total, axis=(0, 1), keepdims=True)
        factor_ref[...] = jnp.broadcast_to(jnp.minimum(1.0, 0.5 * lax.rsqrt(total / count + 1e-30)), factor_ref.shape)


def backward(x, h, dy, weights, gate, up):
    tokens, d = x.shape
    n = gate.shape[0]
    half, q2, q3, columns = d // 2, d // 4, d // 8, T + 128
    hbm = pl.BlockSpec(memory_space=pl.ANY)

    def layer(s):
        return jnp.where(s < n, 1, 0)

    def tile(s):
        return lax.rem(s, n)

    def whole(*shape):
        return pl.BlockSpec(shape, lambda s: (0,) * len(shape), pipeline_mode=pl.Buffered(1))

    later = pl.BlockSpec((1, tokens, T), lambda s: (jnp.maximum(s - n, 0), 0, 0))
    dma = pltpu.SemaphoreType.DMA
    return pl.pallas_call(
        functools.partial(backward_kernel, n, sum(w.size for w in weights)),
        grid=(2 * n,),
        out_shape=(
            jax.ShapeDtypeStruct((2 * n, 2, q3, columns), BF16),
            jax.ShapeDtypeStruct((8, 128), F32),
            jax.ShapeDtypeStruct((max(GATHERED, 1), 2, d, columns), BF16),
        ),
        in_specs=[
            hbm, hbm, hbm,
            pl.BlockSpec((1, d, T), lambda s: (layer(s), 0, tile(s))),
            pl.BlockSpec((1, d, T), lambda s: (layer(s), 0, tile(s))),
            pl.BlockSpec((1, T, d), lambda s: (layer(s), tile(s), 0)),
            later, later,
        ],
        out_specs=(whole(2 * n, 2, q3, columns), whole(8, 128), hbm),
        scratch_shapes=[
            *[pltpu.VMEM((tokens, d), BF16)] * 3,
            pltpu.VMEM((d, tokens), BF16),
            pltpu.VMEM((d, tokens), F32),
            pltpu.VMEM((tokens, T), BF16),
            pltpu.VMEM((tokens, 2 * T), BF16),
            pltpu.VMEM((2, d, columns), F32),
            *[pltpu.VMEM((2, 2, half, columns), BF16)] * 2,
            *[pltpu.VMEM((SLOTS, 2, q2, columns), BF16)] * 2,
            pltpu.VMEM((SLOTS, 2, q2, columns), F32),
            *[pltpu.VMEM((SLOTS, 2, q3, columns), BF16)] * 2,
            pltpu.VMEM((SLOTS, 2, q3, columns), F32),
            pltpu.VMEM((8, columns), F32),
            pltpu.VMEM((8, 8, columns), F32),
            dma((2,)), dma((2, SLOTS)), dma((11, SLOTS)), dma((11, SLOTS)), dma((8,)), dma((8,)),
        ],
        compiler_params=pltpu.CompilerParams(
            dimension_semantics=("arbitrary",), vmem_limit_bytes=VMEM_LIMIT, collective_id=0, has_side_effects=True
        ),
        cost_estimate=pl.CostEstimate(flops=24 * tokens * d * n * T, bytes_accessed=128 << 20, transcendentals=0),
        name="backward_layers",
    )(x, h, dy, *weights, gate, up)


def adamw(w, m, v, g):
    m = 0.9 * m + 0.1 * g
    v = 0.95 * v + 0.05 * g * g
    step = m * lax.rsqrt(v + 1e-8) + 0.1 * w
    return (w - 0.02 * step).astype(BF16), m, v


def optimizer_kernel(pieces, skip, f_ref, *refs):
    gradients, refs = refs[:pieces], refs[pieces:]
    old, outs = refs[:9], refs[-9:]
    factor = f_ref[0:1, 0:1]
    q3 = old[0].shape[1] // 4
    me = lax.axis_index("dp")
    c, y, x = lax.rem(me, 2), lax.rem(me // 2, 2), me // 4

    def update(i, rows, g):
        g = g.astype(F32) * factor
        w, m, v = old[i], old[3 + i], old[6 + i]
        outs[i][0, rows, :], outs[3 + i][0, rows, :], outs[6 + i][0, rows, :] = adamw(
            w[0, rows, :].astype(F32), m[0, rows, :], v[0, rows, :], g
        )

    def share_update(which, share, ref):
        below = 64 * which + 16 * share
        if not isinstance(share, int):
            below = pl.multiple_of(below, 16)
            rows = pl.ds(pl.multiple_of(share * q3, q3), q3)
        else:
            rows = pl.ds(share * q3, q3)
        update(which, rows, ref[:, :T])
        update(2, pl.ds(below, 16), jnp.concatenate([ref[16 * b : 16 * b + 16, T:] for b in range(q3 // 16)], axis=1))

    if pieces == 1:
        for share in range(4):
            for which in range(2):
                share_update(which, share, gradients[0].at[0, which, pl.ds(share * q3, q3)])
        return
    tile = pl.program_id(0) + skip
    for k in range(2):

        @pl.when(pl.program_id(1) == c + k - 2 * k * c)
        def _():
            for i in range(2):
                for j in range(2):
                    px, py = x + i - 2 * i * x, y + j - 2 * j * y
                    for which in range(2):
                        share_update(which, (2 * px + py, 2 * py + px)[which], gradients[4 * i + 2 * j + k].at[tile, which])


def optimizer(first, count, factor, gradients, skip, arrays, so_far):
    _, d, ff = arrays[0].shape
    n = ff // T
    wide = pl.BlockSpec((1, d // 2, T), lambda s, c: (jnp.where(s + first < n, 1, 0), c, lax.rem(s + first, n)))
    tall = pl.BlockSpec((1, T // 2, d), lambda s, c: (jnp.where(s + first < n, 1, 0), 2 * lax.rem(s + first, n) + c, 0))
    three = [wide, wide, tall]
    if len(gradients) == 1:
        taken = pl.BlockSpec((1, 2, d // 2, T + 128), lambda s, c: (s + skip, 0, c, 0))
    else:
        taken = pl.BlockSpec(memory_space=pltpu.VMEM)
    base = 1 + len(gradients) + 9
    return pl.pallas_call(
        functools.partial(optimizer_kernel, len(gradients), skip),
        grid=(count, 2),
        out_shape=tuple(jax.ShapeDtypeStruct(one.shape, one.dtype) for one in arrays),
        in_specs=[
            pl.BlockSpec((8, 128), lambda s, c: (0, 0)),
            *[taken] * len(gradients),
            *three * 3,
            *[pl.BlockSpec(memory_space=pl.ANY)] * len(so_far),
        ],
        out_specs=tuple(three * 3),
        input_output_aliases={base + i: i for i in range(len(so_far))},
        compiler_params=pltpu.CompilerParams(dimension_semantics=("arbitrary", "arbitrary"), vmem_limit_bytes=VMEM_LIMIT),
        cost_estimate=pl.CostEstimate(flops=1 << 20, bytes_accessed=15 * count << 20, transcendentals=0),
        name="optimizer",
    )(factor, *gradients, *arrays, *so_far)


def permute(a, flip):
    return lax.ppermute(a, "dp", [(i, i ^ flip) for i in range(8)])


def solution(mesh):
    def step(x, dy, *arrays):
        weights = arrays[:3]
        x, dy = x[0], dy[0]
        gate, up, h = forward(x, *weights)
        shares, factor, full = backward(x, h, dy, weights, gate, up)
        ahead, first = [], GATHERED
        for size in CHUNKS:
            mine = shares[first : first + size]
            ahead.append([mine, permute(mine, 2), permute(mine, 4), permute(mine, 6)])
            first += size
        new, held, first, count = (), [full], 0, GATHERED
        for here, size in zip(ahead, CHUNKS):
            early = count - LAST
            new = optimizer(first, early, factor, held, 0, arrays, new)
            here, new = lax.optimization_barrier((here, new))
            there = [permute(one, 1) for one in here]
            new = optimizer(first + early, LAST, factor, held, early, arrays, new)
            first, count = first + count, size
            held = [one for pair in zip(here, there) for one in pair]
        return optimizer(first, count, factor, held, 0, arrays, new)

    return jax.shard_map(
        step,
        mesh=mesh,
        in_specs=(P(("rep", "dp"), None, None),) * 2 + (P(None, None, None),) * 9,
        out_specs=(P("rep", None, None),) * 9,
        check_vma=False,
    )
```

```python
import functools

import jax
import jax.numpy as jnp
from jax import lax
from jax.experimental import pallas as pl
from jax.experimental.pallas import tpu as pltpu
from jax.sharding import PartitionSpec as P

MESH = pl.DeviceIdType.MESH
F32, BF16 = jnp.float32, jnp.bfloat16
T = 256
RB = 512
NB = 256
VMEM_LIMIT = 63 * 1024 * 1024
TF = 256
GATHERED = 11
CHUNKS = (5, 4)
SLOTS = 4
LAST = 2


def dot(a, b):
    return jnp.dot(a, b, preferred_element_type=F32)


def dot_nt(a, b):
    return lax.dot_general(a, b, (((1,), (1,)), ((), ())), preferred_element_type=F32)


def dot_tn(a, b):
    return lax.dot_general(a, b, (((0,), (0,)), ((), ())), preferred_element_type=F32)


def norm_scale(wide):
    return lax.rsqrt(jnp.mean(wide * wide, -1, keepdims=True) + 1e-6)


def forward_kernel(x_ref, wg_ref, wu_ref, wd_ref, gate_ref, up_ref, h_ref, a_ref, acc_ref):
    s = pl.program_id(0)
    tokens = x_ref.shape[0]

    @pl.when(s == 0)
    def _():
        def block(i, _):
            rows = pl.ds(pl.multiple_of(i * NB, NB), NB)
            wide = x_ref[rows, :].astype(F32)
            a_ref[rows, :] = (wide * norm_scale(wide)).astype(BF16)
            acc_ref[rows, :] = jnp.zeros((NB, acc_ref.shape[1]), F32)
            return 0

        lax.fori_loop(0, tokens // NB, block, 0)

    wg, wu, wd = wg_ref[0], wu_ref[0], wd_ref[0]
    for r in range(tokens // RB):
        rows = pl.ds(r * RB, RB)
        a = a_ref[rows, :]
        gate = dot(a, wg)
        up = dot(a, wu)
        for part in range(TF // T):
            gate_ref[part, rows, :] = gate[:, part * T : part * T + T]
            up_ref[part, rows, :] = up[:, part * T : part * T + T]
        act = (gate * jax.nn.sigmoid(gate) * up).astype(BF16)
        acc_ref[rows, :] += dot(act, wd)

    @pl.when(s == pl.num_programs(0) - 1)
    def _():
        def block(i, _):
            rows = pl.ds(pl.multiple_of(i * NB, NB), NB)
            h_ref[rows, :] = x_ref[rows, :] + acc_ref[rows, :].astype(BF16)
            return 0

        lax.fori_loop(0, tokens // NB, block, 0)


def forward(x, w_gate, w_up, w_down):
    tokens, d = x.shape
    ff = w_gate.shape[2]
    kept = jax.ShapeDtypeStruct((ff // T, tokens, T), F32)
    keep = pl.BlockSpec((TF // T, tokens, T), lambda s: (s, 0, 0))
    return pl.pallas_call(
        forward_kernel,
        grid=(ff // TF,),
        out_shape=(kept, kept, jax.ShapeDtypeStruct((tokens, d), BF16)),
        in_specs=[
            pl.BlockSpec((tokens, d), lambda s: (0, 0), pipeline_mode=pl.Buffered(1)),
            pl.BlockSpec((1, d, TF), lambda s: (0, 0, s)),
            pl.BlockSpec((1, d, TF), lambda s: (0, 0, s)),
            pl.BlockSpec((1, TF, d), lambda s: (0, s, 0)),
        ],
        out_specs=(keep, keep, pl.BlockSpec((tokens, d), lambda s: (0, 0))),
        scratch_shapes=[pltpu.VMEM((tokens, d), BF16), pltpu.VMEM((tokens, d), F32)],
        compiler_params=pltpu.CompilerParams(dimension_semantics=("arbitrary",), vmem_limit_bytes=VMEM_LIMIT),
        cost_estimate=pl.CostEstimate(flops=6 * tokens * d * ff, bytes_accessed=64 << 20, transcendentals=0),
        name="forward_layer",
    )(x, w_gate, w_up, w_down)


def down_rows(which, share):
    return 128 * (share // 4) + 64 * which + 16 * (share % 4)


def backward_kernel(
    n, count, x_hbm, h_hbm, dy_hbm, wg_ref, wu_ref, wd_ref, gate_ref, up_ref, factor_ref, full, *rest,
):
    chunks, rest = rest[: len(CHUNKS)], rest[len(CHUNKS) :]
    work(n, count, x_hbm, h_hbm, dy_hbm, wg_ref, wu_ref, wd_ref, gate_ref, up_ref, factor_ref, full, chunks, *rest)


def work(
    n, count, x_hbm, h_hbm, dy_hbm, wg_ref, wu_ref, wd_ref, gate_ref, up_ref, factor_ref, full, chunks, share_ref,
    h, d, a, at, dat, act, dgu, g, s1, r1, s2, r2, k2, s3, r3, k3, ssv, ssall,
    load_sem, own_sem, send_sem, recv_sem, ss_send, ss_recv,
):
    s = pl.program_id(0)
    me = lax.axis_index("dp")
    c, y, x = lax.rem(me, 2), lax.rem(me // 2, 2), me // 4
    over_c, over_y, over_x = me + 1 - 2 * c, me + 2 - 4 * y, me + 4 - 8 * x
    tokens, width = h.shape
    half, q2, q3 = width // 2, width // 4, width // 8

    def copy(src, dst, index, slot, target):
        return pltpu.make_async_remote_copy(
            src_ref=src, dst_ref=dst, send_sem=send_sem.at[index, slot], recv_sem=recv_sem.at[index, slot],
            device_id={"dp": target}, device_id_type=MESH,
        )

    def rows_at(start, size):
        return pl.ds(pl.multiple_of(start, size), size)

    def stage1(k):
        slot = lax.rem(k, SLOTS)
        return [copy(s1.at[slot], r1.at[slot], 0, slot, over_c)]

    def stage2(k):
        slot = lax.rem(k, SLOTS)
        return [copy(s2.at[slot, i], r2.at[slot, i], 1 + i, slot, (over_x, over_y)[i]) for i in range(2)]

    def stage3(k):
        slot = lax.rem(k, SLOTS)
        return [copy(s3.at[slot, i], r3.at[slot, i], 3 + i, slot, (over_y, over_x)[i]) for i in range(2)]

    shares = (4 * c + 2 * x + y, 4 * c + 2 * y + x)

    def own(k):
        slot = lax.rem(k, SLOTS)
        return [
            pltpu.make_async_copy(share_ref.at[k, i], full.at[k, i, rows_at(shares[i] * q3, q3)], own_sem.at[i, slot]) for i in range(2)
        ]

    def gather1(k):
        slot = lax.rem(k, SLOTS)
        return [
            copy(share_ref.at[k, i], full.at[k, i, rows_at(shares[i] * q3, q3)], 5 + i, slot, (over_y, over_x)[i]) for i in range(2)
        ]

    def gather2(k):
        slot = lax.rem(k, SLOTS)
        parts = [full.at[k, i, rows_at((2 * c + (x, y)[i]) * q2, q2)] for i in range(2)]
        return [copy(parts[i], parts[i], 7 + i, slot, (over_x, over_y)[i]) for i in range(2)]

    def gather3(k):
        slot = lax.rem(k, SLOTS)
        parts = [full.at[k, i, rows_at(c * half, half)] for i in range(2)]
        return [copy(parts[i], parts[i], 9 + i, slot, over_c) for i in range(2)]

    def start(copies):
        for one in copies:
            one.start()

    def wait(copies):
        for one in copies:
            one.wait()

    def finish(k):
        slot = lax.rem(k, SLOTS)
        for i in range(2):
            one = (k3[slot, i] + r3[slot, i].astype(F32)).astype(BF16)
            share_ref[k, i] = one
            one = one.astype(F32)
            ssv[...] += jnp.sum((one * one).reshape(q3 // 8, 8, one.shape[1]), axis=0)

    def third(k):
        slot = lax.rem(k, SLOTS)
        for i, mine in enumerate((y, x)):
            away, here = rows_at((1 - mine) * q3, q3), rows_at(mine * q3, q3)
            s3[slot, i] = (k2[slot, i, away, :] + r2[slot, i, away, :].astype(F32)).astype(BF16)
            k3[slot, i] = k2[slot, i, here, :] + r2[slot, i, here, :].astype(F32)

    def second(k):
        slot, odd = lax.rem(k, SLOTS), lax.rem(k, 2)
        for i, mine in enumerate((x, y)):
            away, here = rows_at((1 - mine) * q2, q2), rows_at(mine * q2, q2)
            s2[slot, i] = (g[odd, i, rows_at((2 * c + 1 - mine) * q2, q2), :] + r1[slot, i, away, :].astype(F32)).astype(BF16)
            k2[slot, i] = g[odd, i, rows_at((2 * c + mine) * q2, q2), :] + r1[slot, i, here, :].astype(F32)

    def exchange(step):
        def at_tile(early, late, count, f):
            k = jnp.where(step < n + early, step - early, step - late)

            @pl.when(((step < n + early) | (step >= n + late)) & (k >= 0) & (k < count))
            def _():
                f(k)

        at_tile(6, 12, GATHERED, lambda k: wait(gather3(k)))
        at_tile(5, 10, GATHERED, lambda k: (wait(gather2(k)), start(gather3(k))))
        at_tile(4, 8, GATHERED, lambda k: (wait(own(k) + gather1(k)), start(gather2(k))))
        at_tile(3, 6, 2 * n, lambda k: (wait(stage3(k)), finish(k)))
        at_tile(3, 6, GATHERED, lambda k: start(own(k) + gather1(k)))
        at_tile(2, 4, 2 * n, lambda k: (wait(stage2(k)), third(k), start(stage3(k))))
        at_tile(1, 2, 2 * n, lambda k: (wait(stage1(k)), second(k), start(stage2(k))))

    def normed_rows(source, i, _):
        rows = rows_at(i * NB, NB)
        wide = source[rows, :].astype(F32)
        one = (wide * norm_scale(wide)).astype(BF16)
        if source is h:
            a[rows, :] = one
        at[:, rows] = one.T
        return 0

    def load(src, dst, index):
        return pltpu.make_async_copy(src, dst, load_sem.at[index])

    @pl.when(s == 0)
    def _():
        barrier = pltpu.get_barrier_semaphore()
        load(h_hbm, h, 0).start()
        load(dy_hbm, d, 1).start()
        for other in range(1, 8):
            pl.semaphore_signal(barrier, inc=1, device_id={"dp": lax.rem(me + other, 8)}, device_id_type=MESH)
        ssv[...] = jnp.zeros_like(ssv)
        dat[...] = jnp.zeros_like(dat)
        load(h_hbm, h, 0).wait()
        lax.fori_loop(0, tokens // NB, functools.partial(normed_rows, h), 0)
        load(dy_hbm, d, 1).wait()
        pl.semaphore_wait(barrier, 7)

    exchange(s)

    def derive(rows, gate, up, dact):
        sig = jax.nn.sigmoid(gate)
        silu = gate * sig
        dact = dact.astype(BF16).astype(F32)
        act[rows, :] = (silu * up).astype(BF16)
        dgu[rows, :T] = (dact * up * (sig * (1.0 + gate * (1.0 - sig)))).astype(BF16)
        dgu[rows, T:] = (dact * silu).astype(BF16)

    def weight_gradients():
        both = dot(at[...], dgu[...])
        odd = lax.rem(s, 2)
        g[odd, 0, :, :T] = both[:, :T]
        g[odd, 1, :, :T] = both[:, T:]
        down = dot_tn(act[...], d[...])
        for which in range(2):
            for share in range(8):
                row = down_rows(which, share)
                for j in range(width // 128):
                    g[odd, which, share * q3 + 16 * j : share * q3 + 16 * j + 16, T:] = down[row : row + 16, 128 * j : 128 * j + 128]
        s1[lax.rem(s, SLOTS)] = g[odd, :, rows_at((1 - c) * half, half), :].astype(BF16)
        start(stage1(s))

    blocks = [pl.ds(r * RB, RB) for r in range(tokens // RB)]

    @pl.when(s < n)
    def _():
        wgu = jnp.concatenate([wg_ref[0], wu_ref[0]], axis=1)
        wd = wd_ref[0]
        for rows in blocks:
            both = dot(a[rows, :], wgu)
            derive(rows, both[:, :T], both[:, T:], dot_nt(d[rows, :], wd))
        weight_gradients()
        for rows in blocks:
            dat[:, rows] += dot_nt(wgu, dgu[rows, :])

    @pl.when(s >= n)
    def _():
        wd = wd_ref[0]
        for rows in blocks:
            derive(rows, gate_ref[0, rows, :], up_ref[0, rows, :], dot_nt(d[rows, :], wd))
        weight_gradients()

    @pl.when(s == n - 1)
    def _():
        def block(i, _):
            rows = rows_at(i * NB, NB)
            wide = h[rows, :].astype(F32)
            scale = norm_scale(wide)
            by_a = dat[:, rows].T.astype(BF16).astype(F32)
            inner = jnp.mean(by_a * wide, -1, keepdims=True)
            by_h = by_a * scale - wide * (scale * scale * scale * inner)
            d[rows, :] = d[rows, :] + by_h.astype(BF16)
            return 0

        load(x_hbm, a, 0).start()
        lax.fori_loop(0, tokens // NB, block, 0)
        load(x_hbm, a, 0).wait()
        lax.fori_loop(0, tokens // NB, functools.partial(normed_rows, a), 0)

    @pl.when(s == 2 * n - 1)
    def _():
        def drain(step, _):
            exchange(step)
            return 0

        lax.fori_loop(2 * n, max(2 * n + 6, GATHERED + 12), drain, 0)
        ssall[0] = ssv[...]
        first, puts = GATHERED, []
        for i, (chunk, size) in enumerate(zip(chunks, CHUNKS)):
            puts.append(load(share_ref.at[pl.ds(first, size)], chunk, i))
            first += size
        start(puts)
        others = []
        for other in range(1, 8):
            others.append(
                pltpu.make_async_remote_copy(
                    src_ref=ssv, dst_ref=ssall.at[other], send_sem=ss_send.at[other], recv_sem=ss_recv.at[other],
                    device_id={"dp": lax.rem(me + other, 8)}, device_id_type=MESH,
                )
            )
        start(others)
        wait(others)
        wait(puts)
        total = ssall[me]
        for device in range(1, 8):
            total = total + ssall[lax.rem(me - device + 8, 8)]
        total = jnp.sum(total, axis=(0, 1), keepdims=True)
        factor_ref[...] = jnp.broadcast_to(jnp.minimum(1.0, 0.5 * lax.rsqrt(total / count + 1e-30)), factor_ref.shape)


def backward(x, h, dy, weights, gate, up):
    tokens, d = x.shape
    n = gate.shape[0]
    half, q2, q3, columns = d // 2, d // 4, d // 8, T + 128
    hbm = pl.BlockSpec(memory_space=pl.ANY)

    def layer(s):
        return jnp.where(s < n, 1, 0)

    def tile(s):
        return lax.rem(s, n)

    def whole(*shape):
        return pl.BlockSpec(shape, lambda s: (0,) * len(shape), pipeline_mode=pl.Buffered(1))

    later = pl.BlockSpec((1, tokens, T), lambda s: (jnp.maximum(s - n, 0), 0, 0))
    dma = pltpu.SemaphoreType.DMA
    return pl.pallas_call(
        functools.partial(backward_kernel, n, sum(w.size for w in weights)),
        grid=(2 * n,),
        out_shape=(
            jax.ShapeDtypeStruct((8, 128), F32),
            jax.ShapeDtypeStruct((GATHERED, 2, d, columns), BF16),
            *[jax.ShapeDtypeStruct((size, 2, q3, columns), BF16) for size in CHUNKS],
        ),
        in_specs=[
            hbm, hbm, hbm,
            pl.BlockSpec((1, d, T), lambda s: (layer(s), 0, tile(s))),
            pl.BlockSpec((1, d, T), lambda s: (layer(s), 0, tile(s))),
            pl.BlockSpec((1, T, d), lambda s: (layer(s), tile(s), 0)),
            later, later,
        ],
        out_specs=(whole(8, 128), hbm, *[hbm] * len(CHUNKS)),
        scratch_shapes=[
            pltpu.VMEM((2 * n, 2, q3, columns), BF16),
            *[pltpu.VMEM((tokens, d), BF16)] * 3,
            pltpu.VMEM((d, tokens), BF16),
            pltpu.VMEM((d, tokens), F32),
            pltpu.VMEM((tokens, T), BF16),
            pltpu.VMEM((tokens, 2 * T), BF16),
            pltpu.VMEM((2, 2, d, columns), F32),
            *[pltpu.VMEM((SLOTS, 2, half, columns), BF16)] * 2,
            *[pltpu.VMEM((SLOTS, 2, q2, columns), BF16)] * 2,
            pltpu.VMEM((SLOTS, 2, q2, columns), F32),
            *[pltpu.VMEM((SLOTS, 2, q3, columns), BF16)] * 2,
            pltpu.VMEM((SLOTS, 2, q3, columns), F32),
            pltpu.VMEM((8, columns), F32),
            pltpu.VMEM((8, 8, columns), F32),
            dma((2,)), dma((2, SLOTS)), dma((11, SLOTS)), dma((11, SLOTS)), dma((8,)), dma((8,)),
        ],
        compiler_params=pltpu.CompilerParams(
            dimension_semantics=("arbitrary",), vmem_limit_bytes=VMEM_LIMIT, collective_id=0, has_side_effects=True
        ),
        cost_estimate=pl.CostEstimate(flops=24 * tokens * d * n * T, bytes_accessed=128 << 20, transcendentals=0),
        name="backward_layers",
    )(x, h, dy, *weights, gate, up)


def adamw(w, m, v, g):
    m = 0.9 * m + 0.1 * g
    v = 0.95 * v + 0.05 * g * g
    step = m * lax.rsqrt(v + 1e-8) + 0.1 * w
    return (w - 0.02 * step).astype(BF16), m, v


def optimizer_kernel(pieces, skip, f_ref, *refs):
    gradients, refs = refs[:pieces], refs[pieces:]
    old, outs = refs[:9], refs[-9:]
    factor = f_ref[0:1, 0:1]
    q3 = old[0].shape[1] // 4
    me = lax.axis_index("dp")
    c, y, x = lax.rem(me, 2), lax.rem(me // 2, 2), me // 4

    def update(i, rows, g):
        g = g.astype(F32) * factor
        w, m, v = old[i], old[3 + i], old[6 + i]
        outs[i][0, rows, :], outs[3 + i][0, rows, :], outs[6 + i][0, rows, :] = adamw(
            w[0, rows, :].astype(F32), m[0, rows, :], v[0, rows, :], g
        )

    def share_update(which, share, ref):
        below = 64 * which + 16 * share
        if not isinstance(share, int):
            below = pl.multiple_of(below, 16)
            rows = pl.ds(pl.multiple_of(share * q3, q3), q3)
        else:
            rows = pl.ds(share * q3, q3)
        update(which, rows, ref[:, :T])
        update(2, pl.ds(below, 16), jnp.concatenate([ref[16 * b : 16 * b + 16, T:] for b in range(q3 // 16)], axis=1))

    if pieces == 1:
        for share in range(4):
            for which in range(2):
                share_update(which, share, gradients[0].at[0, which, pl.ds(share * q3, q3)])
        return
    tile = pl.program_id(0) + skip
    for k in range(2):

        @pl.when(pl.program_id(1) == c + k - 2 * k * c)
        def _():
            for i in range(2):
                for j in range(2):
                    px, py = x + i - 2 * i * x, y + j - 2 * j * y
                    for which in range(2):
                        share_update(which, (2 * px + py, 2 * py + px)[which], gradients[4 * i + 2 * j + k].at[tile, which])


def optimizer(first, count, factor, gradients, skip, arrays, so_far):
    _, d, ff = arrays[0].shape
    n = ff // T
    wide = pl.BlockSpec((1, d // 2, T), lambda s, c: (jnp.where(s + first < n, 1, 0), c, lax.rem(s + first, n)))
    tall = pl.BlockSpec((1, T // 2, d), lambda s, c: (jnp.where(s + first < n, 1, 0), 2 * lax.rem(s + first, n) + c, 0))
    three = [wide, wide, tall]
    if len(gradients) == 1:
        taken = pl.BlockSpec((1, 2, d // 2, T + 128), lambda s, c: (s + skip, 0, c, 0))
    else:
        taken = pl.BlockSpec(memory_space=pltpu.VMEM)
    base = 1 + len(gradients) + 9
    return pl.pallas_call(
        functools.partial(optimizer_kernel, len(gradients), skip),
        grid=(count, 2),
        out_shape=tuple(jax.ShapeDtypeStruct(one.shape, one.dtype) for one in arrays),
        in_specs=[
            pl.BlockSpec((8, 128), lambda s, c: (0, 0)),
            *[taken] * len(gradients),
            *three * 3,
            *[pl.BlockSpec(memory_space=pl.ANY)] * len(so_far),
        ],
        out_specs=tuple(three * 3),
        input_output_aliases={base + i: i for i in range(len(so_far))},
        compiler_params=pltpu.CompilerParams(dimension_semantics=("arbitrary", "arbitrary"), vmem_limit_bytes=VMEM_LIMIT),
        cost_estimate=pl.CostEstimate(flops=1 << 20, bytes_accessed=15 * count << 20, transcendentals=0),
        name="optimizer",
    )(factor, *gradients, *arrays, *so_far)


def permute(a, flip):
    return lax.ppermute(a, "dp", [(i, i ^ flip) for i in range(8)])


def solution(mesh):
    def step(x, dy, *arrays):
        weights = arrays[:3]
        x, dy = x[0], dy[0]
        gate, up, h = forward(x, *weights)
        factor, full, *chunks = backward(x, h, dy, weights, gate, up)
        ahead = []
        for chunk in chunks:
            here = [chunk]
            for flip in (2, 4, 6):
                here.append(permute(here[0], flip))
            ahead.append(here)
        new, held, first, count = (), [full], 0, GATHERED
        for here, size in zip(ahead, CHUNKS):
            early = count - LAST
            new = optimizer(first, early, factor, held, 0, arrays, new)
            here, new = lax.optimization_barrier((here, new))
            there = [permute(one, 1) for one in here]
            new = optimizer(first + early, LAST, factor, held, early, arrays, new)
            first, count = first + count, size
            held = [one for pair in zip(here, there) for one in pair]
        return optimizer(first, count, factor, held, 0, arrays, new)

    return jax.shard_map(
        step,
        mesh=mesh,
        in_specs=(P(("rep", "dp"), None, None),) * 2 + (P(None, None, None),) * 9,
        out_specs=(P("rep", None, None),) * 9,
        check_vma=False,
    )
```
